128 devices in a mesh: copy: 4 (over z), row: 4 (over x_hi, core), col: 8 (over y, x_lo).
Axes of the slice: x: 4 (x_hi: 2, x_lo: 2; x = x_hi * 2 + x_lo), y: 4, z: 4, core: 2. Of those that a mesh axis runs over, the one named last changes fastest.
Arguments:
- trailing: float32 [32768, 16, 8, 128], P(('copy', 'row'), None, 'col'), parts along dimension 0, may hold values from -6 to 6
- lower_trail: float32 [64, 8, 128, 768], P(('copy', 'row'), None, None, 'col'), parts along dimension 0, may hold values from -0.046875 to 0.046875
- lower_cross: float32 [384, 384], replicated, may hold values from -0.3125 to 0.3125
- panel_inverse: float32 [2, 384, 384], replicated, may hold values from -1 to 1, as said below
- target: float32 [32768, 2, 384], P(('copy', 'row'), None, 'col'), parts along dimension 0, may hold values from -6 to 6
Outputs:
- inverse_panels: float32 [32768, 2, 384], P(('copy', 'row'), None, 'col'), parts along dimension 0
The draws below stay inside these ranges and needn't reach their ends.
There are 4 independent parts, one for each index of `copy`. The reference program is written for one: setup_inputs(seed, part) draws one part's arguments, and reference() takes and returns one part's arrays. A program takes and returns all parts, laid end to end along the dimension named above; an argument that names none is the same for every part. Nothing has to cross between parts.
Inputs may be any that keep to these rules, and one draw needn't show every extreme that they name: `panel_inverse`: each of the two 384 x 384 matrices is unit lower triangular: ones on the diagonal, zeros above it.
All inputs are finite; a program needn't handle non-finite values.
Results may differ from the reference program's by a relative error of at most 0.000071.
Values sent between devices are 32-bit elements; how exact they have to be, the bound alone decides.
A program may use at most 192 MiB of HBM per device.

```python
import jax
import jax.numpy as jnp
from jax import lax

PW = 384
NB = 128
TQ = 16
ROWS = 8192
TRAIL = 16384
N_COL = 8


def draw_panel_inverse(key, part):
    strict_lower = jnp.tril(jnp.ones((PW, PW), jnp.float32), -1)
    values = jax.random.normal(key, (2, PW, PW), jnp.float32) / PW ** 0.5
    values = jnp.clip(values, -1.0, 1.0)
    return values * strict_lower + jnp.eye(PW, dtype=jnp.float32)


def block_scale(rng, shape, pieces, low, high):
    def one(dim, parts):
        draws = jax.random.uniform(jax.random.fold_in(jax.random.fold_in(rng, 6), dim), (parts,), jnp.float32, low / len(pieces), high / len(pieces))
        return jnp.repeat(jnp.exp(draws), shape[dim] // parts).reshape((-1,) + (1,) * (len(shape) - dim - 1))

    loudness = one(*pieces[0])
    for cut in pieces[1:]:
        loudness = loudness * one(*cut)
    return loudness


def normal_values(key, dims, deviation, reach, split=(), kind=jnp.bfloat16):
    array = deviation * jax.random.normal(key, dims, jnp.float32)
    if split:
        array = array * block_scale(key, dims, split, -0.22, 0.18)
    return jnp.clip(array, -reach, reach).astype(kind)


def setup_inputs(seed: int = 0, part: int = 0) -> dict:
    arg_keys = jax.random.split(jax.random.key(seed), 6)
    own_keys = jax.random.split(jax.random.fold_in(arg_keys[5], part), 6)
    return {
        "trailing": normal_values(own_keys[0], (ROWS, TQ, N_COL, NB), 1.0, 6.0, ((0, 4), (2, 8)), jnp.float32),
        "lower_trail": normal_values(own_keys[1], (TQ, N_COL, NB, 2 * PW), TRAIL ** -0.5, 0.046875, ((0, 4), (3, 8)), jnp.float32),
        "lower_cross": normal_values(arg_keys[2], (PW, PW), PW ** -0.5, 0.3125, (), jnp.float32),
        "panel_inverse": draw_panel_inverse(jax.random.fold_in(arg_keys[5], 71), part),
        "target": normal_values(own_keys[4], (ROWS, 2, PW), 1.0, 6.0, ((0, 4), (2, 8)), jnp.float32),
    }


precise = lax.Precision.HIGHEST


def matmul(first, second):
    return jnp.dot(first, second, preferred_element_type=jnp.float32, precision=precise)


def reference(trailing, lower_trail, lower_cross, panel_inverse, target):
    row_count = trailing.shape[0]
    trail_flat = trailing.reshape(row_count, trailing.shape[1] * trailing.shape[2] * trailing.shape[3])
    lower_flat = lower_trail.reshape(trail_flat.shape[1], lower_trail.shape[3])
    update = matmul(trail_flat, lower_flat)
    panel_cols = lower_flat.shape[1] // 2
    right_panel = matmul(target[:, 1, :] - update[:, panel_cols:], panel_inverse[1])
    left_panel = matmul(target[:, 0, :] - update[:, :panel_cols] - matmul(right_panel, lower_cross), panel_inverse[0])
    return jnp.stack([left_panel, right_panel], axis=1)
```

```python
import functools

import jax
import jax.numpy as jnp
from jax import lax
from jax.experimental import pallas as pl
from jax.experimental.pallas import tpu as pltpu
from jax.sharding import PartitionSpec as P

MESH = pl.DeviceIdType.MESH
F32 = jnp.float32
BF16 = jnp.bfloat16
NQ = 4
TILE = 512
N_TILE = 4
Y_OF = ((0, 1), (3, 2))
OFFSETS = [(dx, dy) for dx in range(4) for dy in range(4) if (dx, dy) != (0, 0)]


def split(value):
    high = value.astype(BF16)
    return high, (value - high.astype(F32)).astype(BF16)


def order():
    return [2 * Y_OF[b][a] + x for b in range(2) for a in range(2) for x in range(2)]


def place():
    row, col = lax.axis_index("row"), lax.axis_index("col")
    return row // 2, row % 2, col // 2, col % 2, row, col


def device(x, y, core):
    return {"row": (x // 2) * 2 + core, "col": y * 2 + x % 2}


def kernel(
    trail, low, cross, pinv, tgt, out,
    r_hi, r_lo, stage, slab, acc, lw_hi, lw_lo, in1, in2, in3,
    cross_v, pinv_v, tgt_v, pcp, wl_hi, wl_lo, wr_hi, wr_lo, tw,
    stage_sem, small_sem, send_sem, recv_sem, pass_send, pass_recv, b_send, b_recv, out_sem,
):
    x_hi, core, y, x_lo, row, col = place()
    x = 2 * x_hi + x_lo
    rows = r_hi.shape[0]

    def stage_copy(pos, slot):
        qi, rel, hi = pos // 4, (pos // 2) % 2, pos % 2
        src_row = hi * 2 + (core + rel) % 2
        return pltpu.make_async_copy(
            trail.at[:, src_row * NQ + qi, 0, :], stage.at[slot], stage_sem.at[slot]
        )

    n_stage = stage.shape[0]
    smalls = [
        pltpu.make_async_copy(pinv, pinv_v, small_sem.at[0]),
        pltpu.make_async_copy(cross, cross_v, small_sem.at[1]),
        pltpu.make_async_copy(tgt, tgt_v, small_sem.at[2]),
    ]
    for copy in smalls:
        copy.start()
    for pos in range(n_stage):
        stage_copy(pos, pos).start()

    barrier = pltpu.get_barrier_semaphore()
    for dx, dy in OFFSETS:
        pl.semaphore_signal(
            barrier, inc=1, device_id=device((x + dx) % 4, (y + dy) % 4, core), device_id_type=MESH
        )
    pl.semaphore_signal(barrier, inc=1, device_id=device(x, y, 1 - core), device_id_type=MESH)
    pl.semaphore_wait(barrier, len(OFFSETS) + 1)

    my_slab = slab.at[:, 0, x_hi, pl.ds(pl.multiple_of(col * 96, 96), 96), :]

    def send_low(qi, carry):
        pltpu.make_async_copy(
            low.at[qi, col], my_slab.at[qi], recv_sem.at[qi, x_hi]
        ).start()
        for dx, dy in OFFSETS:
            x2, y2 = (x + dx) % 4, (y + dy) % 4
            pltpu.make_async_remote_copy(
                src_ref=low.at[qi, y2 * 2 + x2 % 2],
                dst_ref=my_slab.at[qi],
                send_sem=send_sem.at[qi],
                recv_sem=recv_sem.at[qi, x_hi],
                device_id=device(x2, y2, core),
                device_id_type=MESH,
            ).start()
        return carry

    lax.fori_loop(0, NQ, send_low, 0)

    for copy in smalls:
        copy.wait()
    exact = functools.partial(
        jnp.dot, preferred_element_type=F32, precision=lax.Precision.HIGHEST
    )
    pcp[...] = exact(exact(pinv_v[1], cross_v[...]), pinv_v[0])
    half = pcp.shape[0]
    left_t = jnp.concatenate([-pinv_v[0].T, pcp[...].T], axis=1)
    wl_hi[...], wl_lo[...] = split(left_t)
    wr_hi[...], wr_lo[...] = split(-pinv_v[1].T)
    own = pl.ds(pl.multiple_of(col * 48, 48), 48)
    own_rows = jnp.concatenate(
        [
            jnp.concatenate([pinv_v[0, own, :], -pcp[own, :]], axis=0),
            jnp.concatenate([jnp.zeros((48, half), F32), pinv_v[1, own, :]], axis=0),
        ],
        axis=1,
    )
    own_hi, own_lo = split(own_rows)
    tw_t = jnp.concatenate(
        [own_hi.astype(F32), own_lo.astype(F32), own_hi.astype(F32)], axis=0
    ).T.astype(BF16)
    for g, c in enumerate(order()):
        for panel in range(2):
            tw[pl.ds(g * 96 + panel * 48, 48), :] = tw_t[panel * half + c * 48 : panel * half + c * 48 + 48]

    acc_flat = acc.reshape(2 * half, rows)

    def start_target(t, carry):
        at = pl.ds(pl.multiple_of(t * TILE, TILE), TILE)
        value = jnp.concatenate([tgt_v[0, :, at], tgt_v[1, :, at]], axis=0)
        high, lowv = split(value)
        rhs = jnp.concatenate([high, high, lowv], axis=0)
        acc_flat[:, at] = jnp.dot(tw[...], rhs, preferred_element_type=F32)
        return carry

    lax.fori_loop(0, N_TILE, start_target, 0)

    def take_stage(pos, carry):
        slot = lax.rem(pos, n_stage)
        stage_copy(pos, slot).wait()
        high, lowv = split(stage[slot])
        at = pl.ds(pl.multiple_of(pos * 128, 128), 128)
        r_hi[:, at] = high
        r_lo[:, at] = lowv

        @pl.when(pos + n_stage < 16)
        def _():
            stage_copy(pos + n_stage, slot).start()

        return carry

    lax.fori_loop(0, 16, take_stage, 0)

    def pass_on(qi, hi):
        return pltpu.make_async_remote_copy(
            src_ref=slab.at[qi, 0, hi],
            dst_ref=slab.at[qi, 1, hi],
            send_sem=pass_send.at[qi, hi],
            recv_sem=pass_recv.at[qi, hi],
            device_id=device(x, y, 1 - core),
            device_id_type=MESH,
        )

    def times_w(qi, rel):
        value = jnp.concatenate([slab[qi, rel, 0], slab[qi, rel, 1]], axis=1)
        high, lowv = split(value)
        at = pl.ds(rel * 256, 256)
        dot = functools.partial(jnp.dot, preferred_element_type=F32)
        left = dot(
            jnp.concatenate([wl_hi[...], wl_lo[...], wl_hi[...]], axis=1),
            jnp.concatenate([high, high, lowv], axis=0),
        )
        right = dot(
            jnp.concatenate([wr_hi[...], wr_lo[...], wr_hi[...]], axis=1),
            jnp.concatenate([high[half:], high[half:], lowv[half:]], axis=0),
        )
        for panel, part in enumerate((left, right)):
            part_hi, part_lo = split(part)
            for g, c in enumerate(order()):
                to = pl.ds(g * 96 + panel * 48, 48)
                lw_hi[to, at] = part_hi[c * 48 : c * 48 + 48]
                lw_lo[to, at] = part_lo[c * 48 : c * 48 + 48]

    def prepare(qi):
        for hi in range(2):
            pltpu.make_async_copy(slab.at[qi, 0, hi], slab.at[qi, 0, hi], recv_sem.at[qi, hi]).wait()
            pass_on(qi, hi).start()
        times_w(qi, 0)
        for hi in range(2):
            pass_on(qi, hi).wait_recv()
        times_w(qi, 1)

    def multiply(qi, t):
        at = pl.ds(pl.multiple_of(t * TILE, TILE), TILE)
        depth = pl.ds(pl.multiple_of(qi * 512, 512), 512)
        lhs = jnp.concatenate([lw_hi[...], lw_lo[...], lw_hi[...]], axis=1)
        high = r_hi[at, depth]
        rhs = jnp.concatenate([high, high, r_lo[at, depth]], axis=1)
        acc_flat[:, at] += lax.dot_general(
            lhs, rhs, (((1,), (1,)), ((), ())), preferred_element_type=F32
        )

    def chunk(qi, carry):
        prepare(qi)

        def tile(t, inner):
            multiply(qi, t)
            return inner

        return lax.fori_loop(0, N_TILE, tile, carry)

    lax.fori_loop(0, NQ - 1, chunk, 0)

    b = y // 2
    a = (y + b) % 2
    x_nbr = device(2 * x_hi + 1 - x_lo, y, core)
    a_nbr = device(x, 3 * b + (1 - 2 * b) * (1 - a), core)
    b_nbr = device(x, 3 * (1 - b) + (2 * b - 1) * a, core)
    every = slice(None)
    sends = (
        ((every, every, 1 - x_lo, 0), (every, 1 - a, x_lo, 0), (1 - b, a, x_lo, 0)),
        ((every, 1 - a, every, 1), (1 - b, a, every, 1), (b, a, 1 - x_lo, 1)),
        ((1 - b, every, every, 2), (b, every, 1 - x_lo, 2), (b, 1 - a, x_lo, 2)),
    )
    keeps = (
        ((every, every, x_lo, 0), (every, a, x_lo, 0), (b, a, x_lo, 0)),
        ((every, a, every, 1), (b, a, every, 1), (b, a, x_lo, 1)),
        ((b, every, every, 2), (b, every, x_lo, 2), (b, a, x_lo, 2)),
    )
    partners = ((x_nbr, a_nbr, b_nbr), (a_nbr, b_nbr, x_nbr), (b_nbr, x_nbr, a_nbr))
    landing = (in1, in2, in3)

    def hop(stage_no, part, t):
        at = pl.ds(pl.multiple_of(t * TILE, TILE), TILE)
        into = landing[stage_no]
        return pltpu.make_async_remote_copy(
            src_ref=acc.at[(*sends[part][stage_no], every, at)],
            dst_ref=into.at[part, ..., at],
            send_sem=b_send.at[stage_no, part, t],
            recv_sem=b_recv.at[stage_no, part, t],
            device_id=partners[part][stage_no],
            device_id_type=MESH,
        )

    def add(stage_no, part, t):
        at = pl.ds(pl.multiple_of(t * TILE, TILE), TILE)
        where = (*keeps[part][stage_no], every, at)
        acc[where] += landing[stage_no][part, ..., at]

    prepare(NQ - 1)

    def last(t, carry):
        multiply(NQ - 1, t)
        for part in range(3):
            hop(0, part, t).start()
        return carry

    lax.fori_loop(0, N_TILE, last, 0)

    for stage_no in range(2):

        def onward(t, carry, stage_no=stage_no):
            for part in range(3):
                hop(stage_no, part, t).wait_recv()
                add(stage_no, part, t)
                hop(stage_no + 1, part, t).start()
            return carry

        lax.fori_loop(0, N_TILE, onward, 0)

    def out_copy(part, t):
        at = pl.ds(pl.multiple_of(t * TILE, TILE), TILE)
        return pltpu.make_async_copy(
            acc.at[b, a, x_lo, part, :, at], out.at[part, :, at], out_sem.at[part, t]
        )

    def finish(t, carry):
        for part in range(3):
            hop(2, part, t).wait_recv()
            add(2, part, t)
            out_copy(part, t).start()
        return carry

    lax.fori_loop(0, N_TILE, finish, 0)

    def drain(t, carry):
        for part in range(3):
            for stage_no in range(3):
                hop(stage_no, part, t).wait_send()
            out_copy(part, t).wait()
        return carry

    lax.fori_loop(0, N_TILE, drain, 0)

    def drain_low(qi, carry):
        sent = slab.at[pl.ds(0, 1), pl.ds(0, 1), :, pl.ds(0, 720), :]
        pltpu.make_async_copy(sent, sent, send_sem.at[qi]).wait()
        for hi in range(2):
            pass_on(qi, hi).wait_send()
        return carry

    lax.fori_loop(0, NQ, drain_low, 0)


def per_device(trailing, lower_trail, lower_cross, panel_inverse, target):
    rows, n_q, _, block = trailing.shape
    width = target.shape[2]
    half = lower_cross.shape[0]
    low = jnp.swapaxes(lower_trail, 2, 3)
    tgt = jnp.transpose(target, (1, 2, 0))
    hbm = pl.BlockSpec(memory_space=pl.ANY)
    dma = pltpu.SemaphoreType.DMA
    out = pl.pallas_call(
        kernel,
        out_shape=jax.ShapeDtypeStruct((3, 32, rows), F32),
        in_specs=[hbm] * 5,
        out_specs=hbm,
        scratch_shapes=[
            pltpu.VMEM((rows, n_q * block), BF16),
            pltpu.VMEM((rows, n_q * block), BF16),
            pltpu.VMEM((4, rows, block), F32),
            pltpu.VMEM((NQ, 2, 2, 2 * half, block), F32),
            pltpu.VMEM((2, 2, 2, 3, 32, rows), F32),
            pltpu.VMEM((2 * half, 4 * block), BF16),
            pltpu.VMEM((2 * half, 4 * block), BF16),
            pltpu.VMEM((3, 2, 2, 32, rows), F32),
            pltpu.VMEM((3, 2, 32, rows), F32),
            pltpu.VMEM((3, 32, rows), F32),
            pltpu.VMEM((half, half), F32),
            pltpu.VMEM((2, half, half), F32),
            pltpu.VMEM((2, width, rows), F32),
            pltpu.VMEM((half, half), F32),
            pltpu.VMEM((half, 2 * half), BF16),
            pltpu.VMEM((half, 2 * half), BF16),
            pltpu.VMEM((half, half), BF16),
            pltpu.VMEM((half, half), BF16),
            pltpu.VMEM((2 * half, 6 * width), BF16),
            dma((4,)),
            dma((3,)),
            dma((NQ,)),
            dma((NQ, 2)),
            dma((NQ, 2)),
            dma((NQ, 2)),
            dma((3, 3, N_TILE)),
            dma((3, 3, N_TILE)),
            dma((3, N_TILE)),
        ],
        compiler_params=pltpu.CompilerParams(
            collective_id=0, has_side_effects=True, vmem_limit_bytes=64 * 1024 * 1024 - 128 * 1024
        ),
    )(trailing, low, lower_cross, panel_inverse, tgt)
    return jnp.transpose(out.reshape(2, width, rows), (2, 0, 1))


def solution(mesh):
    placed = (
        P(("copy", "row"), None, "col", None),
        P(("copy", "row"), None, None, "col"),
        P(),
        P(),
        P(("copy", "row"), None, "col"),
    )
    return jax.shard_map(
        per_device,
        mesh=mesh,
        in_specs=placed,
        out_specs=P(("copy", "row"), None, "col"),
        check_vma=False,
    )
```

```python
import functools

import jax
import jax.numpy as jnp
from jax import lax
from jax.experimental import pallas as pl
from jax.experimental.pallas import tpu as pltpu
from jax.sharding import PartitionSpec as P

MESH = pl.DeviceIdType.MESH
F32 = jnp.float32
BF16 = jnp.bfloat16
NQ = 4
TILE = 512
N_TILE = 4
LEFT, RIGHT = 0, 1
Y_OF = ((0, 1), (3, 2))
ORDERS = (("xab", "abx", "bxa"), ("xab", "abx", "bxa"))
OFFSETS = [(dx, dy) for dx in range(4) for dy in range(4) if (dx, dy) != (0, 0)]
OWNERS = [2 * Y_OF[b][a] + x for b in range(2) for a in range(2) for x in range(2)]


def split(value):
    high = value.astype(BF16)
    return high, (value - high.astype(F32)).astype(BF16)


def device(x, y, core):
    return {"row": (x // 2) * 2 + core, "col": y * 2 + x % 2}


def owner_major(value):
    return jnp.concatenate([value[48 * c : 48 * c + 48] for c in OWNERS], axis=0)


def three(high, low):
    return jnp.concatenate([high, low, high], axis=1)


def kernel(
    trail, low, cross, pinv, tgt, out,
    r_hi, r_lo, stage, slab, acc, lw_hi, lw_lo, in1, in2, in3,
    cross_v, pinv_v, tgt_v, pcp, w_left, w_right, tw,
    stage_sem, small_sem, low_send, low_recv, pass_send, pass_recv, b_send, b_recv,
):
    row, col = lax.axis_index("row"), lax.axis_index("col")
    x_hi, core, y, x_lo = row // 2, row % 2, col // 2, col % 2
    x = 2 * x_hi + x_lo
    rows = r_hi.shape[0]
    half = pcp.shape[0]

    def peer(dx, dy):
        return device((x + dx) % 4, (y + dy) % 4, core)

    partner = device(x, y, 1 - core)

    def remote(src, dst, send, recv, to):
        return pltpu.make_async_remote_copy(
            src_ref=src, dst_ref=dst, send_sem=send, recv_sem=recv, device_id=to, device_id_type=MESH
        )

    def wait_bytes(ref, sem):
        pltpu.make_async_copy(ref, ref, sem).wait()

    barrier = pltpu.get_barrier_semaphore()
    for dx, dy in OFFSETS:
        pl.semaphore_signal(barrier, inc=1, device_id=peer(dx, dy), device_id_type=MESH)
    pl.semaphore_signal(barrier, inc=1, device_id=partner, device_id_type=MESH)

    def stage_copy(pos, slot):
        qi, rel, hi = pos // 4, (pos // 2) % 2, pos % 2
        src_row = hi * 2 + (core + rel) % 2
        return pltpu.make_async_copy(
            trail.at[:, src_row * NQ + qi, 0, :], stage.at[slot], stage_sem.at[slot]
        )

    def span(c):
        return pl.ds(pl.multiple_of(c * 96, 96), 96)

    n_stage = stage.shape[0]
    smalls = [
        pltpu.make_async_copy(pinv, pinv_v, small_sem.at[0]),
        pltpu.make_async_copy(cross, cross_v, small_sem.at[1]),
        pltpu.make_async_copy(tgt, tgt_v, small_sem.at[2]),
    ]
    for copy in smalls:
        copy.start()
    for pos in range(n_stage):
        stage_copy(pos, pos).start()
    def take_stage(pos, carry):
        slot = lax.rem(pos, n_stage)
        stage_copy(pos, slot).wait()
        high, lowv = split(stage[slot])
        at = pl.ds(pl.multiple_of(pos * 128, 128), 128)
        r_hi[:, at] = high
        r_lo[:, at] = lowv

        @pl.when(pos + n_stage < 16)
        def _():
            stage_copy(pos + n_stage, slot).start()

        return carry

    pl.semaphore_wait(barrier, len(OFFSETS) + 1)

    mine_at = slab.at[:, 0, x_hi, span(col)]

    def send_low(qi, carry):
        pltpu.make_async_copy(
            low.at[qi, col], mine_at.at[qi], low_recv.at[y // 2, qi, x_hi]
        ).start()
        for dx, dy in OFFSETS:
            x2, y2 = (x + dx) % 4, (y + dy) % 4
            remote(
                low.at[qi, y2 * 2 + x2 % 2], mine_at.at[qi],
                low_send.at[qi], low_recv.at[y // 2, qi, x_hi], device(x2, y2, core),
            ).start()
        return carry

    lax.fori_loop(0, NQ, send_low, 0)

    for copy in smalls:
        copy.wait()

    exact = functools.partial(
        jnp.dot, preferred_element_type=F32, precision=lax.Precision.HIGHEST
    )
    pcp[...] = exact(exact(pinv_v[1], cross_v[...]), pinv_v[0])
    w_left[...] = three(
        *split(owner_major(jnp.concatenate([-pinv_v[0].T, pcp[...].T], axis=1)))
    )
    w_right[...] = three(*split(owner_major(-pinv_v[1].T)))
    own = pl.ds(pl.multiple_of(col * 48, 48), 48)
    own_rows = jnp.concatenate(
        [
            jnp.concatenate([pinv_v[0, own, :], -pcp[own, :]], axis=0),
            jnp.concatenate([jnp.zeros((48, half), F32), pinv_v[1, own, :]], axis=0),
        ],
        axis=1,
    )
    own_hi, own_lo = split(own_rows)
    tw_t = jnp.concatenate(
        [own_hi.astype(F32), own_lo.astype(F32), own_hi.astype(F32)], axis=0
    ).T
    for panel in range(2):
        tw[pl.ds(panel * half, half), :] = owner_major(
            tw_t[panel * half : (panel + 1) * half]
        ).astype(BF16)

    acc_flat = acc.reshape(2 * half, rows)

    def start_target(t, carry):
        at = pl.ds(pl.multiple_of(t * TILE, TILE), TILE)
        high, lowv = split(jnp.concatenate([tgt_v[0, :, at], tgt_v[1, :, at]], axis=0))
        rhs = jnp.concatenate([high, high, lowv], axis=0)
        acc_flat[:, at] = jnp.dot(tw[...], rhs, preferred_element_type=F32)
        return carry

    lax.fori_loop(0, N_TILE, start_target, 0)

    def pass_on(panel, qi, hi):
        part = pl.ds(panel * half, half)
        return remote(
            slab.at[qi, 0, hi, part], slab.at[qi, 1, hi, part],
            pass_send.at[panel, qi, hi], pass_recv.at[panel, qi, hi], partner,
        )

    def take(panel, qi):
        for hi in range(2):
            wait_bytes(slab.at[qi, 0, hi, pl.ds(0, half)], low_recv.at[panel, qi, hi])
            pass_on(panel, qi, hi).start()

    def take_passed(panel, qi):
        for hi in range(2):
            pass_on(panel, qi, hi).wait_recv()

    def times_w(panel, qi):
        part = pl.ds(panel * half, half) if panel == RIGHT else slice(None)
        value = jnp.concatenate(
            [slab[qi, rel, hi, part] for rel in range(2) for hi in range(2)], axis=1
        )
        high, lowv = split(value)
        lhs = (w_left, w_right)[panel]
        product = jnp.dot(
            lhs[...], jnp.concatenate([high, high, lowv], axis=0), preferred_element_type=F32
        )
        to = pl.ds(panel * half, half)
        lw_hi[to, :], lw_lo[to, :] = split(product)

    def multiply(panels, qi, t):
        at = pl.ds(pl.multiple_of(t * TILE, TILE), TILE)
        depth = pl.ds(pl.multiple_of(qi * 512, 512), 512)
        to = pl.ds(panels[0] * half, len(panels) * half)
        lhs = three(lw_hi[to, :], lw_lo[to, :])
        high = r_hi[at, depth]
        rhs = jnp.concatenate([high, high, r_lo[at, depth]], axis=1)
        acc_flat[to, at] += lax.dot_general(
            lhs, rhs, (((1,), (1,)), ((), ())), preferred_element_type=F32
        )

    b = y // 2
    a = (y + b) % 2
    mine = {"b": b, "a": a, "x": x_lo}
    across = {
        "x": device(2 * x_hi + 1 - x_lo, y, core),
        "a": device(x, 3 * b + (1 - 2 * b) * (1 - a), core),
        "b": device(x, 3 * (1 - b) + (2 * b - 1) * a, core),
    }

    def block(panel, stage_no, part, send):
        index = []
        for pair in "bax":
            turn = ORDERS[panel][part].index(pair)
            if turn > stage_no:
                index.append(slice(None))
            else:
                index.append(1 - mine[pair] if send and turn == stage_no else mine[pair])
        return (panel, *index, part, slice(None))

    landing = (in1, in2, in3)

    def hop(panel, stage_no, part, t):
        at = pl.ds(pl.multiple_of(t * TILE, TILE), TILE)
        return remote(
            acc.at[(*block(panel, stage_no, part, True), at)],
            landing[stage_no].at[panel, part, ..., at],
            b_send.at[panel, stage_no, part, t],
            b_recv.at[panel, stage_no, part, t],
            across[ORDERS[panel][part][stage_no]],
        )

    def onward(panel, stage_no, t):
        at = pl.ds(pl.multiple_of(t * TILE, TILE), TILE)
        for part in range(3):
            hop(panel, stage_no, part, t).wait_recv()
            where = (*block(panel, stage_no, part, False), at)
            acc[where] += landing[stage_no][panel, part, ..., at]
            hop(panel, stage_no + 1, part, t).start()

    def finish(panel, t):
        at = pl.ds(pl.multiple_of(t * TILE, TILE), TILE)
        for part in range(3):
            hop(panel, 2, part, t).wait_recv()
            out[panel, part, :, at] = acc[panel, b, a, x_lo, part, :, at] + in3[panel, part, :, at]

    def tiles(body):
        def step(t, carry):
            body(t)
            return carry

        lax.fori_loop(0, N_TILE, step, 0)

    def start_hops(panel, t):
        for part in range(3):
            hop(panel, 0, part, t).start()

    def chunk(qi, carry):
        take(RIGHT, qi)
        take(LEFT, qi)
        for panel in (RIGHT, LEFT):
            take_passed(panel, qi)
            times_w(panel, qi)
        tiles(lambda t: multiply((LEFT, RIGHT), qi, t))
        return carry

    lax.fori_loop(0, 16, take_stage, 0)
    lax.fori_loop(0, NQ - 1, chunk, 0)

    def end(panel):
        def body(t):
            multiply((panel,), NQ - 1, t)
            start_hops(panel, t)

        return body

    final = NQ - 1
    take(RIGHT, final)
    take(LEFT, final)
    take_passed(RIGHT, final)
    times_w(RIGHT, final)
    tiles(end(RIGHT))
    take_passed(LEFT, final)
    times_w(LEFT, final)
    tiles(end(LEFT))
    for stage_no in range(2):
        for panel in (RIGHT, LEFT):
            tiles(lambda t, panel=panel, stage_no=stage_no: onward(panel, stage_no, t))
    for panel in (RIGHT, LEFT):
        tiles(lambda t, panel=panel: finish(panel, t))

    def drain(t):
        for panel in range(2):
            for part in range(3):
                for stage_no in range(3):
                    hop(panel, stage_no, part, t).wait_send()

    tiles(drain)

    def drain_low(qi, carry):
        wait_bytes(slab.at[pl.ds(0, 1), pl.ds(0, 1), :, pl.ds(0, 720)], low_send.at[qi])
        for panel in range(2):
            for hi in range(2):
                pass_on(panel, qi, hi).wait_send()
        return carry

    lax.fori_loop(0, NQ, drain_low, 0)


def per_device(trailing, lower_trail, lower_cross, panel_inverse, target):
    rows, n_q, _, block = trailing.shape
    width = target.shape[2]
    half = lower_cross.shape[0]
    low = jnp.swapaxes(lower_trail, 2, 3)
    tgt = jnp.transpose(target, (1, 2, 0))
    hbm = pl.BlockSpec(memory_space=pl.ANY)
    dma = pltpu.SemaphoreType.DMA
    out = pl.pallas_call(
        kernel,
        out_shape=pltpu.VMEM((2, 3, 16, rows), F32),
        in_specs=[hbm] * 5,
        out_specs=pl.BlockSpec(memory_space=pltpu.VMEM),
        scratch_shapes=[
            pltpu.VMEM((rows, n_q * block), BF16),
            pltpu.VMEM((rows, n_q * block), BF16),
            pltpu.VMEM((4, rows, block), F32),
            pltpu.VMEM((NQ, 2, 2, 2 * half, block), F32),
            pltpu.VMEM((2, 2, 2, 2, 3, 16, rows), F32),
            pltpu.VMEM((2 * half, 4 * block), BF16),
            pltpu.VMEM((2 * half, 4 * block), BF16),
            pltpu.VMEM((2, 3, 2, 2, 16, rows), F32),
            pltpu.VMEM((2, 3, 2, 16, rows), F32),
            pltpu.VMEM((2, 3, 16, rows), F32),
            pltpu.VMEM((half, half), F32),
            pltpu.VMEM((2, half, half), F32),
            pltpu.VMEM((2, width, rows), F32),
            pltpu.VMEM((half, half), F32),
            pltpu.VMEM((half, 6 * half), BF16),
            pltpu.VMEM((half, 3 * half), BF16),
            pltpu.VMEM((2 * half, 6 * width), BF16),
            dma((4,)),
            dma((3,)),
            dma((NQ,)),
            dma((2, NQ, 2)),
            dma((2, NQ, 2)),
            dma((2, NQ, 2)),
            dma((2, 3, 3, N_TILE)),
            dma((2, 3, 3, N_TILE)),
        ],
        compiler_params=pltpu.CompilerParams(
            collective_id=0, has_side_effects=True, vmem_limit_bytes=56 * 1024 * 1024
        ),
    )(trailing, low, lower_cross, panel_inverse, tgt)
    return jnp.transpose(out.reshape(2, width, rows), (2, 0, 1))


def solution(mesh):
    placed = (
        P(("copy", "row"), None, "col", None),
        P(("copy", "row"), None, None, "col"),
        P(),
        P(),
        P(("copy", "row"), None, "col"),
    )
    return jax.shard_map(
        per_device,
        mesh=mesh,
        in_specs=placed,
        out_specs=P(("copy", "row"), None, "col"),
        check_vma=False,
    )
```

```python
import functools

import jax
import jax.numpy as jnp
from jax import lax
from jax.experimental import pallas as pl
from jax.experimental.pallas import tpu as pltpu
from jax.sharding import PartitionSpec as P

MESH = pl.DeviceIdType.MESH
F32 = jnp.float32
BF16 = jnp.bfloat16
NQ = 4
TILE = 512
N_TILE = 4
LEFT, RIGHT = 0, 1
Y_OF = ((0, 1), (3, 2))
ORDERS = (("xab", "abx", "bxa"), ("xab", "abx", "bxa"))
OFFSETS = [(dx, dy) for dx in range(4) for dy in range(4) if (dx, dy) != (0, 0)]
OWNERS = [2 * Y_OF[b][a] + x for b in range(2) for a in range(2) for x in range(2)]


def split(value):
    high = value.astype(BF16)
    return high, (value - high.astype(F32)).astype(BF16)


def device(x, y, core):
    return {"row": (x // 2) * 2 + core, "col": y * 2 + x % 2}


def owner_major(value):
    return jnp.concatenate([value[48 * c : 48 * c + 48] for c in OWNERS], axis=0)


def three(high, low):
    return jnp.concatenate([high, low, high], axis=1)


def kernel(
    trail, low, cross, pinv, tgt, out,
    r_hi, r_lo, stage, slab, acc, lw_hi, lw_lo, in1, in2, in3,
    cross_v, pinv_v, tgt_v, pcp, w_left, w_right, tw,
    stage_sem, small_sem, low_send, low_recv, pass_send, pass_recv, b_send, b_recv,
):
    row, col = lax.axis_index("row"), lax.axis_index("col")
    x_hi, core, y, x_lo = row // 2, row % 2, col // 2, col % 2
    x = 2 * x_hi + x_lo
    rows = r_hi.shape[0]
    half = pcp.shape[0]

    def peer(dx, dy):
        return device((x + dx) % 4, (y + dy) % 4, core)

    partner = device(x, y, 1 - core)

    def remote(src, dst, send, recv, to):
        return pltpu.make_async_remote_copy(
            src_ref=src, dst_ref=dst, send_sem=send, recv_sem=recv, device_id=to, device_id_type=MESH
        )

    def wait_bytes(ref, sem):
        pltpu.make_async_copy(ref, ref, sem).wait()

    barrier = pltpu.get_barrier_semaphore()
    for dx, dy in OFFSETS:
        pl.semaphore_signal(barrier, inc=1, device_id=peer(dx, dy), device_id_type=MESH)
    pl.semaphore_signal(barrier, inc=1, device_id=partner, device_id_type=MESH)

    def stage_copy(pos, slot):
        qi, rel, hi = pos // 4, (pos // 2) % 2, pos % 2
        src_row = hi * 2 + (core + rel) % 2
        return pltpu.make_async_copy(
            trail.at[:, src_row * NQ + qi, 0, :], stage.at[slot], stage_sem.at[slot]
        )

    def span(c):
        return pl.ds(pl.multiple_of(c * 96, 96), 96)

    n_stage = stage.shape[0]
    smalls = [
        pltpu.make_async_copy(pinv, pinv_v, small_sem.at[0]),
        pltpu.make_async_copy(cross, cross_v, small_sem.at[1]),
        pltpu.make_async_copy(tgt, tgt_v, small_sem.at[2]),
    ]
    for copy in smalls:
        copy.start()
    for pos in range(n_stage):
        stage_copy(pos, pos).start()
    def take_stage(pos, carry):
        slot = lax.rem(pos, n_stage)
        stage_copy(pos, slot).wait()
        high, lowv = split(stage[slot])
        at = pl.ds(pl.multiple_of(pos * 128, 128), 128)
        r_hi[:, at] = high
        r_lo[:, at] = lowv

        @pl.when(pos + n_stage < 16)
        def _():
            stage_copy(pos + n_stage, slot).start()

        return carry

    pl.semaphore_wait(barrier, len(OFFSETS) + 1)

    mine_at = slab.at[:, 0, x_hi, span(col)]

    def send_low(qi, carry):
        pltpu.make_async_copy(
            low.at[qi, col], mine_at.at[qi], low_recv.at[qi, y]
        ).start()
        for dx, dy in OFFSETS:
            x2, y2 = (x + dx) % 4, (y + dy) % 4
            remote(
                low.at[qi, y2 * 2 + x2 % 2], mine_at.at[qi],
                low_send, low_recv.at[qi, y], device(x2, y2, core),
            ).start()
        return carry

    lax.fori_loop(0, NQ, send_low, 0)

    for copy in smalls:
        copy.wait()

    exact = functools.partial(
        jnp.dot, preferred_element_type=F32, precision=lax.Precision.HIGHEST
    )
    pcp[...] = exact(exact(pinv_v[1], cross_v[...]), pinv_v[0])
    w_left[...] = three(
        *split(owner_major(jnp.concatenate([-pinv_v[0].T, pcp[...].T], axis=1)))
    )
    w_right[...] = three(*split(owner_major(-pinv_v[1].T)))
    own = pl.ds(pl.multiple_of(col * 48, 48), 48)
    own_rows = jnp.concatenate(
        [
            jnp.concatenate([pinv_v[0, own, :], -pcp[own, :]], axis=0),
            jnp.concatenate([jnp.zeros((48, half), F32), pinv_v[1, own, :]], axis=0),
        ],
        axis=1,
    )
    own_hi, own_lo = split(own_rows)
    tw_t = jnp.concatenate(
        [own_hi.astype(F32), own_lo.astype(F32), own_hi.astype(F32)], axis=0
    ).T
    for panel in range(2):
        tw[pl.ds(panel * half, half), :] = owner_major(
            tw_t[panel * half : (panel + 1) * half]
        ).astype(BF16)

    acc_flat = acc.reshape(2 * half, rows)

    def start_target(t, carry):
        at = pl.ds(pl.multiple_of(t * TILE, TILE), TILE)
        high, lowv = split(jnp.concatenate([tgt_v[0, :, at], tgt_v[1, :, at]], axis=0))
        rhs = jnp.concatenate([high, high, lowv], axis=0)
        acc_flat[:, at] = jnp.dot(tw[...], rhs, preferred_element_type=F32)
        return carry

    lax.fori_loop(0, N_TILE, start_target, 0)

    def piece(qi, rel, ys):
        return slab.at[qi, rel, :, pl.ds(192 * ys, 192)]

    def pass_on(qi, ys):
        return remote(piece(qi, 0, ys), piece(qi, 1, ys), pass_send, pass_recv.at[qi, ys], partner)

    def sources(panel):
        return 2 * panel, 2 * panel + 1

    def take(panel, qi):
        for ys in sources(panel):
            wait_bytes(piece(qi, 0, ys), low_recv.at[qi, ys])
            pass_on(qi, ys).start()

    def take_passed(panel, qi):
        for ys in sources(panel):
            pass_on(qi, ys).wait_recv()

    def times_w(panel, qi):
        part = pl.ds(panel * half, half) if panel == RIGHT else slice(None)
        value = jnp.concatenate(
            [slab[qi, rel, hi, part] for rel in range(2) for hi in range(2)], axis=1
        )
        high, lowv = split(value)
        lhs = (w_left, w_right)[panel]
        product = jnp.dot(
            lhs[...], jnp.concatenate([high, high, lowv], axis=0), preferred_element_type=F32
        )
        to = pl.ds(panel * half, half)
        lw_hi[to, :], lw_lo[to, :] = split(product)

    def multiply(panels, qi, t):
        at = pl.ds(pl.multiple_of(t * TILE, TILE), TILE)
        depth = pl.ds(pl.multiple_of(qi * 512, 512), 512)
        to = pl.ds(panels[0] * half, len(panels) * half)
        lhs = three(lw_hi[to, :], lw_lo[to, :])
        high = r_hi[at, depth]
        rhs = jnp.concatenate([high, high, r_lo[at, depth]], axis=1)
        acc_flat[to, at] += lax.dot_general(
            lhs, rhs, (((1,), (1,)), ((), ())), preferred_element_type=F32
        )

    b = y // 2
    a = (y + b) % 2
    mine = {"b": b, "a": a, "x": x_lo}
    across = {
        "x": device(2 * x_hi + 1 - x_lo, y, core),
        "a": device(x, 3 * b + (1 - 2 * b) * (1 - a), core),
        "b": device(x, 3 * (1 - b) + (2 * b - 1) * a, core),
    }

    def block(panel, stage_no, part, send):
        index = []
        for pair in "bax":
            turn = ORDERS[panel][part].index(pair)
            if turn > stage_no:
                index.append(slice(None))
            else:
                index.append(1 - mine[pair] if send and turn == stage_no else mine[pair])
        return (panel, *index, part, slice(None))

    landing = (in1, in2, in3)

    def hop(panel, stage_no, part, t):
        at = pl.ds(pl.multiple_of(t * TILE, TILE), TILE)
        return remote(
            acc.at[(*block(panel, stage_no, part, True), at)],
            landing[stage_no].at[panel, part, ..., at],
            b_send,
            b_recv.at[panel, stage_no, t],
            across[ORDERS[panel][part][stage_no]],
        )

    def onward(panel, stage_no, t):
        at = pl.ds(pl.multiple_of(t * TILE, TILE), TILE)
        wait_bytes(landing[stage_no].at[panel, ..., at], b_recv.at[panel, stage_no, t])
        for part in range(3):
            where = (*block(panel, stage_no, part, False), at)
            acc[where] += landing[stage_no][panel, part, ..., at]
            hop(panel, stage_no + 1, part, t).start()

    def finish(panel, t):
        at = pl.ds(pl.multiple_of(t * TILE, TILE), TILE)
        wait_bytes(in3.at[panel, ..., at], b_recv.at[panel, 2, t])
        for part in range(3):
            out[panel, part, :, at] = acc[panel, b, a, x_lo, part, :, at] + in3[panel, part, :, at]

    def tiles(body):
        def step(t, carry):
            body(t)
            return carry

        lax.fori_loop(0, N_TILE, step, 0)

    def start_hops(panel, t):
        for part in range(3):
            hop(panel, 0, part, t).start()

    def chunk(qi, carry):
        for panel in (RIGHT, LEFT):
            take_passed(panel, qi)
            times_w(panel, qi)

        def tile(t):
            multiply((LEFT, RIGHT), qi, t)

            @pl.when(t == 2)
            def _():
                take(RIGHT, qi + 1)
                take(LEFT, qi + 1)

        tiles(tile)
        return carry

    lax.fori_loop(0, 16, take_stage, 0)
    take(RIGHT, 0)
    take(LEFT, 0)
    lax.fori_loop(0, NQ - 1, chunk, 0)

    def end(panel):
        def body(t):
            multiply((panel,), NQ - 1, t)
            start_hops(panel, t)

        return body

    final = NQ - 1
    take_passed(RIGHT, final)
    times_w(RIGHT, final)
    tiles(end(RIGHT))
    take_passed(LEFT, final)
    times_w(LEFT, final)
    tiles(end(LEFT))
    for stage_no in range(2):
        for panel in (RIGHT, LEFT):
            tiles(lambda t, panel=panel, stage_no=stage_no: onward(panel, stage_no, t))
    for panel in (RIGHT, LEFT):
        tiles(lambda t, panel=panel: finish(panel, t))

    wait_bytes(acc_flat.at[pl.ds(0, 7 * half // 4)], b_send)
    wait_bytes(slab.at[pl.ds(0, 2), :, :, pl.ds(0, 720)], low_send)
    wait_bytes(slab.at[pl.ds(0, 2)], pass_send)


def per_device(trailing, lower_trail, lower_cross, panel_inverse, target):
    rows, n_q, _, block = trailing.shape
    width = target.shape[2]
    half = lower_cross.shape[0]
    low = jnp.swapaxes(lower_trail, 2, 3)
    tgt = jnp.transpose(target, (1, 2, 0))
    hbm = pl.BlockSpec(memory_space=pl.ANY)
    dma = pltpu.SemaphoreType.DMA
    out = pl.pallas_call(
        kernel,
        out_shape=pltpu.VMEM((2, 3, 16, rows), F32),
        in_specs=[hbm] * 5,
        out_specs=pl.BlockSpec(memory_space=pltpu.VMEM),
        scratch_shapes=[
            pltpu.VMEM((rows, n_q * block), BF16),
            pltpu.VMEM((rows, n_q * block), BF16),
            pltpu.VMEM((4, rows, block), F32),
            pltpu.VMEM((NQ, 2, 2, 2 * half, block), F32),
            pltpu.VMEM((2, 2, 2, 2, 3, 16, rows), F32),
            pltpu.VMEM((2 * half, 4 * block), BF16),
            pltpu.VMEM((2 * half, 4 * block), BF16),
            pltpu.VMEM((2, 3, 2, 2, 16, rows), F32),
            pltpu.VMEM((2, 3, 2, 16, rows), F32),
            pltpu.VMEM((2, 3, 16, rows), F32),
            pltpu.VMEM((half, half), F32),
            pltpu.VMEM((2, half, half), F32),
            pltpu.VMEM((2, width, rows), F32),
            pltpu.VMEM((half, half), F32),
            pltpu.VMEM((half, 6 * half), BF16),
            pltpu.VMEM((half, 3 * half), BF16),
            pltpu.VMEM((2 * half, 6 * width), BF16),
            dma((4,)),
            dma((3,)),
            dma(()),
            dma((NQ, 4)),
            dma(()),
            dma((NQ, 4)),
            dma(()),
            dma((2, 3, N_TILE)),
        ],
        compiler_params=pltpu.CompilerParams(
            collective_id=0, has_side_effects=True, vmem_limit_bytes=56 * 1024 * 1024
        ),
    )(trailing, low, lower_cross, panel_inverse, tgt)
    return jnp.transpose(out.reshape(2, width, rows), (2, 0, 1))


def solution(mesh):
    placed = (
        P(("copy", "row"), None, "col", None),
        P(("copy", "row"), None, None, "col"),
        P(),
        P(),
        P(("copy", "row"), None, "col"),
    )
    return jax.shard_map(
        per_device,
        mesh=mesh,
        in_specs=placed,
        out_specs=P(("copy", "row"), None, "col"),
        check_vma=False,
    )
```

```python
import functools

import jax
import jax.numpy as jnp
from jax import lax
from jax.experimental import pallas as pl
from jax.experimental.pallas import tpu as pltpu
from jax.sharding import PartitionSpec as P

MESH = pl.DeviceIdType.MESH
F32 = jnp.float32
BF16 = jnp.bfloat16
NQ = 4
TILE = 512
N_TILE = 4
LEFT, RIGHT = 0, 1
Y_OF = ((0, 1), (3, 2))
ORDERS = (("xab", "abx", "bxa"), ("xab", "abx", "bxa"))
OFFSETS = [(dx, dy) for dx in range(4) for dy in range(4) if (dx, dy) != (0, 0)]
OWNERS = [2 * Y_OF[b][a] + x for b in range(2) for a in range(2) for x in range(2)]


def split(value):
    high = value.astype(BF16)
    return high, (value - high.astype(F32)).astype(BF16)


def device(x, y, core):
    return {"row": (x // 2) * 2 + core, "col": y * 2 + x % 2}


def owner_major(value):
    return jnp.concatenate([value[48 * c : 48 * c + 48] for c in OWNERS], axis=0)


def three(high, low):
    return jnp.concatenate([high, low, high], axis=1)


def kernel(
    trail, low, cross, pinv, tgt, out,
    r_hi, r_lo, stage, slab, acc, lw_hi, lw_lo, in1, in2, in3,
    cross_v, pinv_v, tgt_v, pcp, w_left, w_right, tw,
    stage_sem, small_sem, low_send, low_recv, pass_send, pass_recv, b_send, b_recv,
):
    row, col = lax.axis_index("row"), lax.axis_index("col")
    x_hi, core, y, x_lo = row // 2, row % 2, col // 2, col % 2
    x = 2 * x_hi + x_lo
    rows = r_hi.shape[0]
    half = pcp.shape[0]

    def peer(dx, dy):
        return device((x + dx) % 4, (y + dy) % 4, core)

    partner = device(x, y, 1 - core)

    def remote(src, dst, send, recv, to):
        return pltpu.make_async_remote_copy(
            src_ref=src, dst_ref=dst, send_sem=send, recv_sem=recv, device_id=to, device_id_type=MESH
        )

    def wait_bytes(ref, sem):
        pltpu.make_async_copy(ref, ref, sem).wait()

    barrier = pltpu.get_barrier_semaphore()
    for dx, dy in OFFSETS:
        pl.semaphore_signal(barrier, inc=1, device_id=peer(dx, dy), device_id_type=MESH)
    pl.semaphore_signal(barrier, inc=1, device_id=partner, device_id_type=MESH)

    def stage_copy(pos, slot):
        qi, rel, hi = pos // 4, (pos // 2) % 2, pos % 2
        src_row = hi * 2 + (core + rel) % 2
        return pltpu.make_async_copy(
            trail.at[:, src_row * NQ + qi, 0, :], stage.at[slot], stage_sem.at[slot]
        )

    def span(c):
        return pl.ds(pl.multiple_of(c * 96, 96), 96)

    n_stage = stage.shape[0]
    smalls = [
        pltpu.make_async_copy(pinv, pinv_v, small_sem.at[0]),
        pltpu.make_async_copy(cross, cross_v, small_sem.at[1]),
        pltpu.make_async_copy(tgt, tgt_v, small_sem.at[2]),
    ]
    for copy in smalls:
        copy.start()
    for pos in range(n_stage):
        stage_copy(pos, pos).start()
    def take_stage(pos, carry):
        slot = lax.rem(pos, n_stage)
        stage_copy(pos, slot).wait()
        high, lowv = split(stage[slot])
        at = pl.ds(pl.multiple_of(pos * 128, 128), 128)
        r_hi[:, at] = high
        r_lo[:, at] = lowv

        @pl.when(pos + n_stage < 16)
        def _():
            stage_copy(pos + n_stage, slot).start()

        return carry

    pl.semaphore_wait(barrier, len(OFFSETS) + 1)

    mine_at = slab.at[:, 0, x_hi, span(col)]

    def send_low(qi, carry):
        pltpu.make_async_copy(
            low.at[qi, col], mine_at.at[qi], low_recv.at[qi, y]
        ).start()
        for dx, dy in OFFSETS:
            x2, y2 = (x + dx) % 4, (y + dy) % 4
            remote(
                low.at[qi, y2 * 2 + x2 % 2], mine_at.at[qi],
                low_send, low_recv.at[qi, y], device(x2, y2, core),
            ).start()
        return carry

    lax.fori_loop(0, NQ, send_low, 0)

    for copy in smalls:
        copy.wait()

    exact = functools.partial(
        jnp.dot, preferred_element_type=F32, precision=lax.Precision.HIGHEST
    )
    pcp[...] = exact(exact(pinv_v[1], cross_v[...]), pinv_v[0])
    w_left[...] = three(
        *split(owner_major(jnp.concatenate([-pinv_v[0].T, pcp[...].T], axis=1)))
    )
    w_right[...] = three(*split(owner_major(-pinv_v[1].T)))
    own = pl.ds(pl.multiple_of(col * 48, 48), 48)
    own_rows = jnp.concatenate(
        [
            jnp.concatenate([pinv_v[0, own, :], -pcp[own, :]], axis=0),
            jnp.concatenate([jnp.zeros((48, half), F32), pinv_v[1, own, :]], axis=0),
        ],
        axis=1,
    )
    own_hi, own_lo = split(own_rows)
    tw_t = jnp.concatenate(
        [own_hi.astype(F32), own_lo.astype(F32), own_hi.astype(F32)], axis=0
    ).T
    for panel in range(2):
        tw[pl.ds(panel * half, half), :] = owner_major(
            tw_t[panel * half : (panel + 1) * half]
        ).astype(BF16)

    acc_flat = acc.reshape(2 * half, rows)

    def start_target(t, carry):
        at = pl.ds(pl.multiple_of(t * TILE, TILE), TILE)
        high, lowv = split(jnp.concatenate([tgt_v[0, :, at], tgt_v[1, :, at]], axis=0))
        rhs = jnp.concatenate([high, high, lowv], axis=0)
        acc_flat[:, at] = jnp.dot(tw[...], rhs, preferred_element_type=F32)
        return carry

    lax.fori_loop(0, N_TILE, start_target, 0)

    def piece(qi, rel, ys):
        return slab.at[qi, rel, :, pl.ds(192 * ys, 192)]

    def pass_on(qi, ys):
        return remote(piece(qi, 0, ys), piece(qi, 1, ys), pass_send, pass_recv.at[qi, ys], partner)

    def sources(panel):
        return 2 * panel, 2 * panel + 1

    def take(panel, qi):
        for ys in sources(panel):
            wait_bytes(piece(qi, 0, ys), low_recv.at[qi, ys])
            pass_on(qi, ys).start()

    def take_passed(panel, qi):
        for ys in sources(panel):
            pass_on(qi, ys).wait_recv()

    def times_w(panel, qi):
        part = pl.ds(panel * half, half) if panel == RIGHT else slice(None)
        value = jnp.concatenate(
            [slab[qi, rel, hi, part] for rel in range(2) for hi in range(2)], axis=1
        )
        high, lowv = split(value)
        lhs = (w_left, w_right)[panel]
        product = jnp.dot(
            lhs[...], jnp.concatenate([high, high, lowv], axis=0), preferred_element_type=F32
        )
        to = pl.ds(panel * half, half)
        lw_hi[to, :], lw_lo[to, :] = split(product)

    def multiply(panels, qi, t):
        at = pl.ds(pl.multiple_of(t * TILE, TILE), TILE)
        depth = pl.ds(pl.multiple_of(qi * 512, 512), 512)
        to = pl.ds(panels[0] * half, len(panels) * half)
        lhs = three(lw_hi[to, :], lw_lo[to, :])
        high = r_hi[at, depth]
        rhs = jnp.concatenate([high, high, r_lo[at, depth]], axis=1)
        acc_flat[to, at] += lax.dot_general(
            lhs, rhs, (((1,), (1,)), ((), ())), preferred_element_type=F32
        )

    b = y // 2
    a = (y + b) % 2
    mine = {"b": b, "a": a, "x": x_lo}
    across = {
        "x": device(2 * x_hi + 1 - x_lo, y, core),
        "a": device(x, 3 * b + (1 - 2 * b) * (1 - a), core),
        "b": device(x, 3 * (1 - b) + (2 * b - 1) * a, core),
    }

    def block(panel, stage_no, part, send):
        index = []
        for pair in "bax":
            turn = ORDERS[panel][part].index(pair)
            if turn > stage_no:
                index.append(slice(None))
            else:
                index.append(1 - mine[pair] if send and turn == stage_no else mine[pair])
        return (panel, *index, part, slice(None))

    landing = (in1, in2, in3)

    def hop(panel, stage_no, part, t):
        at = pl.ds(pl.multiple_of(t * TILE, TILE), TILE)
        return remote(
            acc.at[(*block(panel, stage_no, part, True), at)],
            landing[stage_no].at[panel, part, ..., at],
            b_send,
            b_recv.at[panel, stage_no, t],
            across[ORDERS[panel][part][stage_no]],
        )

    def onward(panel, stage_no, t):
        at = pl.ds(pl.multiple_of(t * TILE, TILE), TILE)
        wait_bytes(landing[stage_no].at[panel, ..., at], b_recv.at[panel, stage_no, t])
        for part in range(3):
            where = (*block(panel, stage_no, part, False), at)
            acc[where] += landing[stage_no][panel, part, ..., at]
            hop(panel, stage_no + 1, part, t).start()

    def finish(panel, t):
        at = pl.ds(pl.multiple_of(t * TILE, TILE), TILE)
        wait_bytes(in3.at[panel, ..., at], b_recv.at[panel, 2, t])
        for part in range(3):
            out[panel, part, :, at] = acc[panel, b, a, x_lo, part, :, at] + in3[panel, part, :, at]

    def tiles(body):
        def step(t, carry):
            body(t)
            return carry

        lax.fori_loop(0, N_TILE, step, 0)

    def start_hops(panel, t):
        for part in range(3):
            hop(panel, 0, part, t).start()

    def chunk(qi, carry):
        for panel in (RIGHT, LEFT):
            take_passed(panel, qi)
            times_w(panel, qi)

        def tile(t):
            multiply((LEFT, RIGHT), qi, t)

            @pl.when(t == 1)
            def _():
                take(RIGHT, qi + 1)

            @pl.when(t == 2)
            def _():
                take(LEFT, qi + 1)

        tiles(tile)
        return carry

    lax.fori_loop(0, 16, take_stage, 0)
    take(RIGHT, 0)
    take(LEFT, 0)
    lax.fori_loop(0, NQ - 1, chunk, 0)

    def end(panel):
        def body(t):
            multiply((panel,), NQ - 1, t)
            start_hops(panel, t)

        return body

    final = NQ - 1
    take_passed(RIGHT, final)
    times_w(RIGHT, final)
    tiles(end(RIGHT))
    take_passed(LEFT, final)
    times_w(LEFT, final)
    tiles(end(LEFT))
    for stage_no in range(2):
        for panel in (RIGHT, LEFT):
            tiles(lambda t, panel=panel, stage_no=stage_no: onward(panel, stage_no, t))
    for panel in (RIGHT, LEFT):
        tiles(lambda t, panel=panel: finish(panel, t))

    wait_bytes(acc_flat.at[pl.ds(0, 7 * half // 4)], b_send)
    wait_bytes(slab.at[pl.ds(0, 2), :, :, pl.ds(0, 720)], low_send)
    wait_bytes(slab.at[pl.ds(0, 2)], pass_send)


def per_device(trailing, lower_trail, lower_cross, panel_inverse, target):
    rows, n_q, _, block = trailing.shape
    width = target.shape[2]
    half = lower_cross.shape[0]
    low = jnp.swapaxes(lower_trail, 2, 3)
    tgt = jnp.transpose(target, (1, 2, 0))
    hbm = pl.BlockSpec(memory_space=pl.ANY)
    dma = pltpu.SemaphoreType.DMA
    out = pl.pallas_call(
        kernel,
        out_shape=pltpu.VMEM((2, 3, 16, rows), F32),
        in_specs=[hbm] * 5,
        out_specs=pl.BlockSpec(memory_space=pltpu.VMEM),
        scratch_shapes=[
            pltpu.VMEM((rows, n_q * block), BF16),
            pltpu.VMEM((rows, n_q * block), BF16),
            pltpu.VMEM((4, rows, block), F32),
            pltpu.VMEM((NQ, 2, 2, 2 * half, block), F32),
            pltpu.VMEM((2, 2, 2, 2, 3, 16, rows), F32),
            pltpu.VMEM((2 * half, 4 * block), BF16),
            pltpu.VMEM((2 * half, 4 * block), BF16),
            pltpu.VMEM((2, 3, 2, 2, 16, rows), F32),
            pltpu.VMEM((2, 3, 2, 16, rows), F32),
            pltpu.VMEM((2, 3, 16, rows), F32),
            pltpu.VMEM((half, half), F32),
            pltpu.VMEM((2, half, half), F32),
            pltpu.VMEM((2, width, rows), F32),
            pltpu.VMEM((half, half), F32),
            pltpu.VMEM((half, 6 * half), BF16),
            pltpu.VMEM((half, 3 * half), BF16),
            pltpu.VMEM((2 * half, 6 * width), BF16),
            dma((4,)),
            dma((3,)),
            dma(()),
            dma((NQ, 4)),
            dma(()),
            dma((NQ, 4)),
            dma(()),
            dma((2, 3, N_TILE)),
        ],
        compiler_params=pltpu.CompilerParams(
            collective_id=0, has_side_effects=True, vmem_limit_bytes=56 * 1024 * 1024
        ),
    )(trailing, low, lower_cross, panel_inverse, tgt)
    return jnp.transpose(out.reshape(2, width, rows), (2, 0, 1))


def solution(mesh):
    placed = (
        P(("copy", "row"), None, "col", None),
        P(("copy", "row"), None, None, "col"),
        P(),
        P(),
        P(("copy", "row"), None, "col"),
    )
    return jax.shard_map(
        per_device,
        mesh=mesh,
        in_specs=placed,
        out_specs=P(("copy", "row"), None, "col"),
        check_vma=False,
    )
```
